256 devices in a mesh: groups: 2 (over y), ep: 128 (over x, z, core).
Axes of the slice: x: 4, y: 2, z: 16, core: 2. Of those that a mesh axis runs over, the one named last changes fastest.
The devices are a block of a 4x16x16 slice.
Arguments:
- tokens: bfloat16 [1024, 7168], P(('groups', 'ep')), parts along dimension 0, may hold values from -6 to 6
- routes: int32 [1024, 8], P(('groups', 'ep')), parts along dimension 0, may hold values from 0 to 15, as said below
- gates: float32 [1024, 8], P(('groups', 'ep')), parts along dimension 0, may hold values from 0.05 to 0.6
- gate_weight: bfloat16 [7168, 32768], P(None, 'ep'), may hold values from -0.0625 to 0.0625
- up_weight: bfloat16 [7168, 32768], P(None, 'ep'), may hold values from -0.0625 to 0.0625
- down_weight: bfloat16 [32768, 7168], P('ep'), may hold values from -0.125 to 0.125
Outputs:
- mixed: bfloat16 [1024, 7168], P(('groups', 'ep')), parts along dimension 0
The draws below stay inside these ranges and needn't reach their ends.
There are 2 independent parts, one for each index of `groups`. The reference program is written for one: setup_inputs(seed, part) draws one part's arguments, and reference() takes and returns one part's arrays. A program takes and returns all parts, laid end to end along the dimension named above; an argument that names none is the same for every part. Nothing has to cross between parts.
Inputs may be any that keep to these rules, and one draw needn't show every extreme that they name: `routes`: each token names 8 different experts. Among the 4 tokens of one device no expert is named by more than 3 of them, and in every draw one expert is named by exactly 3 tokens of every device.
All inputs are finite; a program needn't handle non-finite values.
Results may differ from the reference program's by a relative error of at most 0.0085.
Values may be sent and summed in bfloat16 or wider, within the bound.
No kernel may reach another device: no remote copies, remote signals or barrier semaphores. Data moves between devices by JAX's collectives and lax.ppermute only.
A program may use at most 128 MiB of HBM per device.

```python
import math
import jax
import jax.numpy as jnp
from jax import lax

D = 7168
FF = 2048
TOP = 8
EXPERTS = 16
TOK_DEV = 4
CAP = 3
TOKENS = 512


def draw_routes(key, part):
    hot_expert = jax.random.randint(jax.random.fold_in(key, 11), (), 0, EXPERTS).astype(jnp.int32)
    blocks = TOKENS // TOK_DEV
    block_keys = jax.random.split(jax.random.fold_in(key, 12), blocks)
    others = (hot_expert + 1 + jnp.arange(EXPERTS - 1, dtype=jnp.int32)) % EXPERTS
    expert_pool = jnp.repeat(others, CAP)

    def one_block(block_key):
        key_pool, key_rows, key_cols = jax.random.split(block_key, 3)
        shuffled = expert_pool[jax.random.permutation(key_pool, expert_pool.shape[0])]
        chosen = jnp.concatenate([jnp.full((CAP,), hot_expert, jnp.int32), shuffled[:TOK_DEV * TOP - CAP]])
        ordered = jnp.sort(chosen)
        route_table = ordered.reshape(TOP, TOK_DEV).T
        route_table = route_table[jax.random.permutation(key_rows, TOK_DEV)]
        scores = jax.random.randint(key_cols, (TOK_DEV, TOP), 0, 1 << 20) * TOP + jnp.arange(TOP, dtype=jnp.int32)[None, :]
        return jnp.take_along_axis(route_table, jnp.argsort(scores, axis=1), axis=1)
    return jax.vmap(one_block)(block_keys).reshape(TOKENS, TOP).astype(jnp.int32)


def level_of(rng, dims, cuts, low, top_value):
    level = 1.0
    for dim, blocks in cuts:
        draws = jax.random.uniform(jax.random.fold_in(jax.random.fold_in(rng, 6), dim), (blocks,), jnp.float32, low / len(cuts), top_value / len(cuts))
        level = level * jnp.repeat(jnp.exp(draws), dims[dim] // blocks).reshape((-1,) + (1,) * (len(dims) - 1 - dim))
    return level


def gaussian(key, dims, deviation, most, cuts=(), kind=jnp.bfloat16):
    gain = level_of(key, dims, cuts, -0.22, 0.18) if cuts else 1.0
    entries = jax.random.normal(key, dims, jnp.float32) * deviation * gain
    return jnp.minimum(jnp.maximum(entries, -most), most).astype(kind)


def setup_inputs(seed: int = 0, part: int = 0) -> dict:
    streams_of = jax.random.split(jax.random.key(seed), 7)
    part_splits = jax.random.split(jax.random.fold_in(streams_of[6], part), 7)
    return {
        "tokens": gaussian(part_splits[0], (TOKENS, D), 1.0, 6.0, ((0, 128),)),
        "routes": draw_routes(jax.random.fold_in(jax.random.fold_in(streams_of[6], part), 71), part),
        "gates": jnp.clip(jnp.exp(math.log(0.6) - 2.4849067 * jax.random.uniform(part_splits[2], (TOKENS, TOP), jnp.float32) ** level_of(part_splits[2], (TOKENS, TOP), ((0, 128),), -0.2, 0.2)), 0.05, 0.6),
        "gate_weight": gaussian(streams_of[3], (D, EXPERTS * FF), D ** -0.5, 0.0625, ((1, 128),)),
        "up_weight": gaussian(streams_of[4], (D, EXPERTS * FF), D ** -0.5, 0.0625, ((1, 128),)),
        "down_weight": gaussian(streams_of[5], (EXPERTS * FF, D), FF ** -0.5, 0.125, ((0, 128),)),
    }


def reference(tokens, routes, gates, gate_weight, up_weight, down_weight):
    bound = CAP * (TOKENS // TOK_DEV)

    def add_expert(running, expert):
        matches = routes == expert
        routed = jnp.any(matches, axis=1)
        weight = jnp.sum(jnp.where(matches, gates, jnp.zeros_like(gates)), axis=1)
        row_order = jnp.argsort(jnp.where(routed, 0, 1).astype(jnp.int32), stable=True)[:bound].astype(jnp.int32)
        picked_rows = tokens[row_order]
        start = (expert * FF).astype(jnp.int32)
        gate_cols = lax.dynamic_slice_in_dim(gate_weight, start, FF, 1)
        up_cols = lax.dynamic_slice_in_dim(up_weight, start, FF, 1)
        down_rows = lax.dynamic_slice_in_dim(down_weight, start, FF, 0)
        gate_act = jnp.dot(picked_rows, gate_cols, preferred_element_type=jnp.float32)
        up_act = jnp.dot(picked_rows, up_cols, preferred_element_type=jnp.float32)
        hidden = (jax.nn.silu(gate_act) * up_act).astype(jnp.bfloat16)
        expert_out = jnp.dot(hidden, down_rows, preferred_element_type=jnp.float32)
        running = running.at[row_order].add(weight[row_order][:, None] * expert_out)
        return running, None

    initial = jnp.zeros(tokens.shape, jnp.float32)
    running, unused = lax.scan(add_expert, initial, jnp.arange(EXPERTS, dtype=jnp.int32))
    return running.astype(jnp.bfloat16)
```

```python
import jax
import jax.numpy as jnp
from jax import lax
from jax.sharding import Mesh
from jax.sharding import PartitionSpec as P

EXPERTS = 16
LANES = 128
EP = ("ep_0", "ep_1", "ep_2")
GROUPS_EP = ("groups", "ep_0", "ep_1", "ep_2")
FAR = (8, 4, 12)
X_OFFSETS = (1, 3, 2)


def take_from(value, axis, offset):
    count = lax.axis_size(axis)
    return lax.ppermute(value, axis, [((i + offset) % count, i) for i in range(count)])


def give_to(value, axis, offset):
    count = lax.axis_size(axis)
    return lax.ppermute(value, axis, [(i, (i + offset) % count) for i in range(count)])


def gate_columns(routes, gates):
    member = routes[:, :, None] == jnp.arange(EXPERTS, dtype=routes.dtype)
    left = jnp.sum(jnp.where(member, gates[:, :, None], 0.0), axis=1)
    parts = []
    for _ in range(3):
        part = lax.reduce_precision(left, 8, 7)
        parts.append(part.astype(jnp.bfloat16))
        left = left - part
    columns = jnp.concatenate(parts, axis=1)
    return jnp.pad(columns, ((0, 0), (0, LANES - columns.shape[1])))


def weight_of(columns, expert):
    index = jnp.arange(LANES, dtype=jnp.int32)
    mine = (index % EXPERTS == expert) & (index < 3 * EXPERTS)
    return jnp.sum(jnp.where(mine, columns.astype(jnp.float32), 0.0), axis=1, keepdims=True)


def gathered_over_chips(rows):
    half = 2 * rows.shape[0]
    far = jnp.concatenate([rows] + [take_from(rows, "ep_1", k) for k in FAR], axis=0)
    near = jnp.concatenate(
        [far, take_from(far, "ep_1", 1), take_from(far, "ep_1", -1)]
        + [take_from(far[:half], "ep_1", k) for k in (2, -2)],
        axis=0,
    )
    return jnp.concatenate([near] + [take_from(near, "ep_0", k) for k in X_OFFSETS], axis=0)


def scattered_over_chips(rows):
    low, high = jnp.bfloat16, jnp.float32
    count = rows.shape[0] // 4
    pieces = [rows[i * count : (i + 1) * count] for i in range(4)]
    near = pieces[0]
    for piece, k in zip(pieces[1:], X_OFFSETS):
        near = near + give_to(piece.astype(low), "ep_0", k).astype(high)
    count = count // 4
    far = near[:count]
    for i, k in ((1, 1), (2, -1)):
        far = far + give_to(near[i * count : (i + 1) * count].astype(low), "ep_1", k).astype(high)
    half = count // 2
    top = far[:half]
    for i, k in ((6, 2), (7, -2)):
        top = top + give_to(near[i * half : (i + 1) * half].astype(low), "ep_1", k).astype(high)
    far = jnp.concatenate([top, far[half:]], axis=0)
    count = count // 4
    mine = far[:count]
    for i, k in enumerate(FAR):
        piece = far[(i + 1) * count : (i + 2) * count]
        mine = mine + give_to(piece.astype(low), "ep_1", k).astype(high)
    return mine


def shards(tokens, routes, gates, gate_weight, up_weight, down_weight):
    width = tokens.shape[1]
    cores = [(i, i ^ 1) for i in range(lax.axis_size("ep_2"))]
    expert = lax.axis_index(EP) // (lax.axis_size(EP) // EXPERTS)

    def hidden_of(rows):
        gate_act = jnp.dot(rows[:, :width], gate_weight, preferred_element_type=jnp.float32)
        up_act = jnp.dot(rows[:, :width], up_weight, preferred_element_type=jnp.float32)
        return (jax.nn.silu(gate_act) * up_act).astype(jnp.bfloat16)

    def partial_of(hidden, rows):
        result = jnp.dot(hidden, down_weight, preferred_element_type=jnp.float32)
        return result * weight_of(rows[:, width:], expert)

    rows = jnp.concatenate([tokens, gate_columns(routes, gates)], axis=1)
    own = gathered_over_chips(rows)
    other = lax.ppermute(own, "ep_2", cores)
    own_hidden = hidden_of(own)
    other_partial = partial_of(hidden_of(other), other).astype(jnp.bfloat16)
    returned = lax.ppermute(other_partial, "ep_2", cores)
    total = partial_of(own_hidden, own) + returned.astype(jnp.float32)
    return scattered_over_chips(total).astype(jnp.bfloat16)


def solution(mesh):
    torus = Mesh(
        mesh.devices.reshape(mesh.shape["groups"], 4, 16, 2), ("groups", "ep_0", "ep_1", "ep_2")
    )
    placed = (
        P(GROUPS_EP, None),
        P(GROUPS_EP, None),
        P(GROUPS_EP, None),
        P(None, EP),
        P(None, EP),
        P(EP, None),
    )
    return jax.shard_map(
        shards, mesh=torus, in_specs=placed, out_specs=P(GROUPS_EP, None), check_vma=False
    )
```

```python
import functools

import jax
import jax.numpy as jnp
from jax import lax
from jax.experimental import pallas as pl
from jax.experimental.pallas import tpu as pltpu
from jax.sharding import Mesh
from jax.sharding import PartitionSpec as P


EXPERTS = 16
LANES = 128
EP = ("ep_0", "ep_1", "ep_2")
GROUPS_EP = ("groups", "ep_0", "ep_1", "ep_2")
X_OFFSETS = (1, 3, 2)
FAR = (8, 4, 12)
Z_OFFSETS = (0, 8, 4, 12, 1, 9, 5, 13, 15, 7, 3, 11, 2, 10, 14, 6)
LOW, HIGH = jnp.bfloat16, jnp.float32


def take_from(value, axis, offset):
    count = lax.axis_size(axis)
    return lax.ppermute(value, axis, [((i + offset) % count, i) for i in range(count)])


def give_to(value, axis, offset):
    count = lax.axis_size(axis)
    return lax.ppermute(value, axis, [(i, (i + offset) % count) for i in range(count)])


def other_core(value):
    return give_to(value, "ep_2", 1)


def gate_columns(routes, gates):
    member = routes[:, :, None] == jnp.arange(EXPERTS, dtype=routes.dtype)
    left = jnp.sum(jnp.where(member, gates[:, :, None], 0.0), axis=1)
    parts = []
    for _ in range(3):
        part = lax.reduce_precision(left, 8, 7)
        parts.append(part.astype(LOW))
        left = left - part
    columns = jnp.concatenate(parts, axis=1)
    return jnp.pad(columns, ((0, 0), (0, LANES - columns.shape[1])))


def row_order(tok_rows):
    count = lax.axis_size("ep_1")
    wanted = (lax.axis_index("ep_1") + jnp.array(Z_OFFSETS, jnp.int32)) % count
    wanted = (wanted[:, None] * tok_rows + jnp.arange(tok_rows, dtype=jnp.int32)).reshape(-1)
    return (wanted[:, None] == jnp.arange(count * tok_rows, dtype=jnp.int32)).astype(LOW)


def hidden_kernel(steps, expert_ref, order_ref, *refs):
    b_refs, a_refs, c_refs = refs[:4], refs[4:8], refs[8:12]
    gate_ref, up_ref, hidden_ref, weight_ref, gate_sum, up_sum = refs[12:]
    step = pl.program_id(0)

    @pl.when(step == 0)
    def _():
        gate_sum[...] = jnp.zeros_like(gate_sum)
        up_sum[...] = jnp.zeros_like(up_sum)

    def add(rows):
        gate_sum[...] += jnp.dot(rows, gate_ref[...], preferred_element_type=HIGH)
        up_sum[...] += jnp.dot(rows, up_ref[...], preferred_element_type=HIGH)

    @pl.when(step < steps)
    def _():
        add(jnp.concatenate([r[...] for r in b_refs], axis=0))

    @pl.when(step >= steps)
    def _():
        add(jnp.concatenate([r[...] for r in a_refs], axis=0))

    @pl.when(step == pl.num_programs(0) - 1)
    def _():
        gate_act = gate_sum[...]
        hidden = (gate_act / (1.0 + jnp.exp(-gate_act)) * up_sum[...]).astype(LOW)
        order = order_ref[...]
        count = order.shape[0]
        index = lax.broadcasted_iota(jnp.int32, (count, LANES), 1)
        mine = (lax.rem(index, EXPERTS) == expert_ref[0]) & (index < 3 * EXPERTS)
        for i in range(4):
            part = hidden[i * count : (i + 1) * count]
            moved = jnp.dot(order, part, preferred_element_type=HIGH)
            hidden_ref[i * count : (i + 1) * count, :] = moved.astype(LOW)
            columns = jnp.dot(order, c_refs[i][...], preferred_element_type=HIGH)
            weight = jnp.sum(jnp.where(mine, columns, 0.0), axis=1, keepdims=True)
            weight_ref[i * count : (i + 1) * count, :] = jnp.broadcast_to(weight, (count, LANES))


def hidden_of(expert, order, b_blocks, a_rows, gate_weight, up_weight):
    count = order.shape[0]
    units = gate_weight.shape[1]
    a_width = a_rows.shape[1] // 4
    b_width = b_blocks[0].shape[1] - LANES
    chunk = a_width // 2
    a_steps, b_steps = a_width // chunk, b_width // chunk

    def b_index(k):
        return 0, jnp.minimum(k, b_steps - 1)

    def a_index(i):
        return lambda k: (0, i * a_steps + jnp.maximum(k - b_steps, 0))

    def w_index(k):
        return lax.rem(k + a_steps, a_steps + b_steps), 0

    whole = lambda k: (0, 0)
    return pl.pallas_call(
        functools.partial(hidden_kernel, b_steps),
        grid=(a_steps + b_steps,),
        in_specs=[
            pl.BlockSpec(memory_space=pltpu.SMEM),
            pl.BlockSpec((count, count), whole),
            *[pl.BlockSpec((count, chunk), b_index) for _ in range(4)],
            *[pl.BlockSpec((count, chunk), a_index(i)) for i in range(4)],
            *[pl.BlockSpec((count, LANES), lambda k: (0, b_width // LANES)) for _ in range(4)],
            pl.BlockSpec((chunk, units), w_index),
            pl.BlockSpec((chunk, units), w_index),
        ],
        out_specs=[
            pl.BlockSpec((4 * count, units), whole),
            pl.BlockSpec((4 * count, LANES), whole),
        ],
        out_shape=[
            jax.ShapeDtypeStruct((4 * count, units), LOW),
            jax.ShapeDtypeStruct((4 * count, LANES), HIGH),
        ],
        scratch_shapes=[pltpu.VMEM((4 * count, units), HIGH) for _ in range(2)],
        cost_estimate=pl.CostEstimate(
            flops=2 * 4 * count * (a_width + b_width) * 2 * units,
            bytes_accessed=2 * (a_width + b_width) * (4 * count + 2 * units),
            transcendentals=4 * count * units,
        ),
        name="hidden",
    )(expert, order, *b_blocks, *([a_rows] * 4), *b_blocks, gate_weight, up_weight)


def partial_kernel(steps, hidden_ref, weight_ref, down_ref, b_ref, a_ref):
    step = pl.program_id(0)
    result = jnp.dot(hidden_ref[...], down_ref[...], preferred_element_type=HIGH)
    result = (result * weight_ref[:, :1]).astype(LOW)

    @pl.when(step < steps)
    def _():
        b_ref[...] = result

    @pl.when(step >= steps)
    def _():
        a_ref[...] = result.reshape(a_ref.shape)


def total_kernel(steps, hidden_ref, weight_ref, down_ref, from_b, from_a, *refs):
    b_outs, a_outs = refs[:4], refs[4:]
    step = pl.program_id(0)
    result = jnp.dot(hidden_ref[...], down_ref[...], preferred_element_type=HIGH)
    result = result * weight_ref[:, :1]
    count = b_outs[0].shape[0]

    @pl.when(step < steps)
    def _():
        total = result + from_b[...].astype(HIGH)
        for i, ref in enumerate(b_outs):
            ref[...] = total[i * count : (i + 1) * count].astype(ref.dtype)

    @pl.when(step >= steps)
    def _():
        for i in range(4):
            total = result[i * count : (i + 1) * count] + from_a[i].astype(HIGH)
            at = 0
            for ref in a_outs:
                ref[i] = total[at : at + ref.shape[1]].astype(ref.dtype)
                at += ref.shape[1]


def down_call(hidden, weight, down_weight, a_width, received=None):
    rows, units = hidden.shape
    count, b_width = rows // 4, down_weight.shape[1] - a_width
    chunk = a_width // 2
    a_steps, b_steps = a_width // chunk, b_width // chunk
    whole = lambda k: (0, 0)
    b_index = lambda k: (0, jnp.minimum(k, b_steps - 1))
    a_index = lambda k: (0, 0, jnp.maximum(k - b_steps, 0))
    in_specs = [
        pl.BlockSpec((rows, units), whole),
        pl.BlockSpec((rows, LANES), whole),
        pl.BlockSpec((units, chunk), lambda k: (0, lax.rem(k + a_steps, a_steps + b_steps))),
    ]
    b_block = pl.BlockSpec((rows, chunk), b_index)
    a_block = pl.BlockSpec((4, count, chunk), a_index)
    args = (hidden, weight, down_weight)
    if received is None:
        body = partial_kernel
        out_specs = [b_block, a_block]
        out_shape = [
            jax.ShapeDtypeStruct((rows, b_width), LOW),
            jax.ShapeDtypeStruct((4, count, a_width), LOW),
        ]
    else:
        body = total_kernel
        in_specs += [b_block, a_block]
        args += tuple(received)
        cuts = [(count // 4, HIGH), (count // 4, LOW), (count // 4, LOW)] + [(count // 8, LOW)] * 2
        out_specs = [pl.BlockSpec((count, chunk), b_index) for _ in range(4)]
        out_specs += [pl.BlockSpec((4, n, chunk), a_index) for n, _ in cuts]
        out_shape = [jax.ShapeDtypeStruct((count, b_width), t) for t in (HIGH, LOW, LOW, LOW)]
        out_shape += [jax.ShapeDtypeStruct((4, n, a_width), t) for n, t in cuts]
    return pl.pallas_call(
        functools.partial(body, b_steps),
        grid=(a_steps + b_steps,),
        in_specs=in_specs,
        out_specs=out_specs,
        out_shape=out_shape,
        cost_estimate=pl.CostEstimate(
            flops=2 * rows * units * (a_width + b_width),
            bytes_accessed=2 * (a_width + b_width) * (units + 2 * rows),
            transcendentals=0,
        ),
        name="partial" if received is None else "total",
    )(*args)


def near_sum(kept, pieces):
    got = []
    for piece, k in zip(pieces, (1, -1, 2, -2)):
        got.append(give_to(piece, "ep_1", k))
    total = kept + got[0].astype(HIGH) + got[1].astype(HIGH)
    half = got[2].shape[-2]
    top = total[..., :half, :] + got[2].astype(HIGH) + got[3].astype(HIGH)
    return jnp.concatenate([top, total[..., half:, :]], axis=-2)


def far_sum(rows):
    count = rows.shape[-2] // 4
    total = rows[..., :count, :]
    for i, k in enumerate(FAR):
        piece = rows[..., (i + 1) * count : (i + 2) * count, :]
        total = total + give_to(piece.astype(LOW), "ep_1", k).astype(HIGH)
    return total


def layer(tokens, routes, gates, gate_weight, up_weight, down_weight):
    tok_rows, width = tokens.shape
    a_width = width // 4
    expert = lax.axis_index(EP) // (lax.axis_size(EP) // EXPERTS)
    expert = expert.astype(jnp.int32).reshape(1)
    order = row_order(tok_rows)

    a_own = tokens[:, :a_width]
    b_own = jnp.concatenate([tokens[:, a_width:], gate_columns(routes, gates)], axis=1)
    a_lanes = jnp.concatenate([a_own] + [take_from(a_own, "ep_0", k) for k in X_OFFSETS], axis=1)
    b_near = lax.all_gather(b_own, "ep_1", axis=0, tiled=True)
    a_lanes, b_near = lax.optimization_barrier((a_lanes, b_near))
    b_mine = [b_near] + [take_from(b_near, "ep_0", k) for k in X_OFFSETS]
    b_other = [other_core(block) for block in b_mine]
    a_mine = lax.all_gather(a_lanes, "ep_1", axis=0, tiled=True)
    a_other = other_core(a_mine)

    hidden, weight = hidden_of(expert, order, b_other, a_other, gate_weight, up_weight)
    sent = down_call(hidden, weight, down_weight, a_width)
    received = [other_core(value) for value in sent]
    hidden, weight = hidden_of(expert, order, b_mine, a_mine, gate_weight, up_weight)
    pieces = down_call(hidden, weight, down_weight, a_width, received)

    b_total = pieces[0]
    for i, k in enumerate(X_OFFSETS):
        got = give_to(pieces[i + 1], "ep_0", k)
        b_total = b_total + got.astype(HIGH)
    a_total = far_sum(near_sum(pieces[4], pieces[5:]))
    a_result = a_total[0]
    for i, k in enumerate(X_OFFSETS):
        a_result = a_result + give_to(a_total[i + 1].astype(LOW), "ep_0", k).astype(HIGH)
    n = b_total.shape[0] // 8
    cut = [b_total[i * n : j * n].astype(LOW) for i, j in ((2, 4), (4, 6), (6, 7), (7, 8))]
    b_result = far_sum(near_sum(b_total[: 2 * n], cut))
    return jnp.concatenate([a_result, b_result], axis=1).astype(LOW)


def solution(mesh):
    torus = Mesh(
        mesh.devices.reshape(mesh.shape["groups"], 4, 16, 2), ("groups", "ep_0", "ep_1", "ep_2")
    )
    placed = (
        P(GROUPS_EP, None),
        P(GROUPS_EP, None),
        P(GROUPS_EP, None),
        P(None, EP),
        P(None, EP),
        P(EP, None),
    )
    return jax.shard_map(
        layer, mesh=torus, in_specs=placed, out_specs=P(GROUPS_EP, None), check_vma=False
    )
```

```python
import functools

import jax
import jax.numpy as jnp
from jax import lax
from jax.experimental import pallas as pl
from jax.experimental.pallas import tpu as pltpu
from jax.sharding import Mesh
from jax.sharding import PartitionSpec as P


EXPERTS = 16
LANES = 128
EP = ("ep_0", "ep_1", "ep_2")
GROUPS_EP = ("groups", "ep_0", "ep_1", "ep_2")
FAR = (8, 4, 12)
Z_OFFSETS = (0, 8, 4, 12, 1, 9, 5, 13, 15, 7, 3, 11, 2, 10, 14, 6)
LOW, HIGH = jnp.bfloat16, jnp.float32


def take_from(value, axis, offset):
    count = lax.axis_size(axis)
    return lax.ppermute(value, axis, [((i + offset) % count, i) for i in range(count)])


def give_to(value, axis, offset):
    count = lax.axis_size(axis)
    return lax.ppermute(value, axis, [(i, (i + offset) % count) for i in range(count)])


def other_core(value):
    return give_to(value, "ep_2", 1)


def gate_columns(routes, gates):
    member = routes[:, :, None] == jnp.arange(EXPERTS, dtype=routes.dtype)
    left = jnp.sum(jnp.where(member, gates[:, :, None], 0.0), axis=1)
    parts = []
    for _ in range(3):
        part = lax.reduce_precision(left, 8, 7)
        parts.append(part.astype(LOW))
        left = left - part
    columns = jnp.concatenate(parts, axis=1)
    return jnp.pad(columns, ((0, 0), (0, LANES - columns.shape[1])))


def row_order(tok_rows):
    count = lax.axis_size("ep_1")
    wanted = (lax.axis_index("ep_1") + jnp.array(Z_OFFSETS, jnp.int32)) % count
    wanted = (wanted[:, None] * tok_rows + jnp.arange(tok_rows, dtype=jnp.int32)).reshape(-1)
    return (wanted[:, None] == jnp.arange(count * tok_rows, dtype=jnp.int32)).astype(LOW)


def hidden_kernel(blocks, expert_ref, order_ref, *refs):
    row_refs, column_refs = refs[:blocks], refs[blocks : 2 * blocks]
    gate_ref, up_ref, hidden_ref, weight_ref, gate_sum, up_sum = refs[2 * blocks :]
    step = pl.program_id(0)

    @pl.when(step == 0)
    def _():
        gate_sum[...] = jnp.zeros_like(gate_sum)
        up_sum[...] = jnp.zeros_like(up_sum)

    rows = jnp.concatenate([r[...] for r in row_refs], axis=0)
    gate_sum[...] += jnp.dot(rows, gate_ref[...], preferred_element_type=HIGH)
    up_sum[...] += jnp.dot(rows, up_ref[...], preferred_element_type=HIGH)

    @pl.when(step == pl.num_programs(0) - 1)
    def _():
        gate_act = gate_sum[...]
        hidden = (gate_act / (1.0 + jnp.exp(-gate_act)) * up_sum[...]).astype(LOW)
        columns = jnp.concatenate([r[...] for r in column_refs], axis=0)
        order = order_ref[...]
        count = order.shape[0]
        index = lax.broadcasted_iota(jnp.int32, (count, LANES), 1)
        mine = (lax.rem(index, EXPERTS) == expert_ref[0]) & (index < 3 * EXPERTS)
        for at in range(0, hidden.shape[0], count):
            moved = jnp.dot(order, hidden[at : at + count], preferred_element_type=HIGH)
            hidden_ref[at : at + count, :] = moved.astype(LOW)
            moved = jnp.dot(order, columns[at : at + count], preferred_element_type=HIGH)
            weight = jnp.sum(jnp.where(mine, moved, 0.0), axis=1, keepdims=True)
            weight_ref[at : at + count, :] = jnp.broadcast_to(weight, (count, LANES))


def hidden_of(expert, order, blocks, gate_weight, up_weight):
    width, units = gate_weight.shape
    chunk = width // 4
    rows = sum(block.shape[0] for block in blocks)
    whole = lambda k: (0, 0)
    return pl.pallas_call(
        functools.partial(hidden_kernel, len(blocks)),
        grid=(width // chunk,),
        in_specs=[
            pl.BlockSpec(memory_space=pltpu.SMEM),
            pl.BlockSpec(order.shape, whole),
            *[pl.BlockSpec((block.shape[0], chunk), lambda k: (0, k)) for block in blocks],
            *[pl.BlockSpec((block.shape[0], LANES), lambda k: (0, width // LANES)) for block in blocks],
            pl.BlockSpec((chunk, units), lambda k: (k, 0)),
            pl.BlockSpec((chunk, units), lambda k: (k, 0)),
        ],
        out_specs=[pl.BlockSpec((rows, units), whole), pl.BlockSpec((rows, LANES), whole)],
        out_shape=[
            jax.ShapeDtypeStruct((rows, units), LOW),
            jax.ShapeDtypeStruct((rows, LANES), HIGH),
        ],
        scratch_shapes=[pltpu.VMEM((rows, units), HIGH) for _ in range(2)],
        cost_estimate=pl.CostEstimate(
            flops=2 * rows * width * 2 * units,
            bytes_accessed=2 * width * (rows + 2 * units),
            transcendentals=rows * units,
        ),
        name="hidden",
    )(expert, order, *blocks, *blocks, gate_weight, up_weight)


def partial_kernel(hidden_ref, weight_ref, down_ref, mine_ref, other_ref):
    result = jnp.dot(hidden_ref[...], down_ref[...], preferred_element_type=HIGH)
    result = result * weight_ref[:, :1]
    count = mine_ref.shape[0]
    mine_ref[...] = result[:count]
    other_ref[...] = result[count:].astype(LOW)


def partial_of(hidden, weight, down_weight):
    rows, units = hidden.shape
    width = down_weight.shape[1]
    chunk = width // 4
    whole = lambda k: (0, 0)
    half = pl.BlockSpec((rows // 2, chunk), lambda k: (0, k))
    return pl.pallas_call(
        partial_kernel,
        grid=(width // chunk,),
        in_specs=[
            pl.BlockSpec((rows, units), whole),
            pl.BlockSpec((rows, LANES), whole),
            pl.BlockSpec((units, chunk), lambda k: (0, k)),
        ],
        out_specs=[half, half],
        out_shape=[jax.ShapeDtypeStruct((rows // 2, width), t) for t in (HIGH, LOW)],
        cost_estimate=pl.CostEstimate(
            flops=2 * rows * units * width,
            bytes_accessed=2 * width * (units + 2 * rows),
            transcendentals=0,
        ),
        name="partial",
    )(hidden, weight, down_weight)


def near_sum(kept, pieces):
    got = []
    for piece, k in zip(pieces, (1, -1, 2, -2)):
        got.append(give_to(piece, "ep_1", k))
    total = kept + got[0].astype(HIGH) + got[1].astype(HIGH)
    half = got[2].shape[-2]
    top = total[..., :half, :] + got[2].astype(HIGH) + got[3].astype(HIGH)
    return jnp.concatenate([top, total[..., half:, :]], axis=-2)


def far_sum(rows):
    count = rows.shape[-2] // 4
    total = rows[..., :count, :]
    for i, k in enumerate(FAR):
        piece = rows[..., (i + 1) * count : (i + 2) * count, :]
        total = total + give_to(piece.astype(LOW), "ep_1", k).astype(HIGH)
    return total


def layer(tokens, routes, gates, gate_weight, up_weight, down_weight):
    expert = lax.axis_index(EP) // (lax.axis_size(EP) // EXPERTS)
    expert = expert.astype(jnp.int32).reshape(1)
    order = row_order(tokens.shape[0])

    def hidden_and_partial(blocks):
        with_core = blocks + [other_core(block) for block in blocks]
        hidden = hidden_of(expert, order, with_core, gate_weight, up_weight)

        def partial():
            return partial_of(*hidden, down_weight)

        return partial

    own = jnp.concatenate([tokens, gate_columns(routes, gates)], axis=1)
    near = lax.all_gather(own, "ep_1", axis=0, tiled=True)
    half = near.shape[0] // 2
    up = take_from(near, "ep_0", 1)
    down = take_from(near, "ep_0", -1)
    far_up = take_from(up[:half], "ep_0", 1)
    far_down = take_from(down[half:], "ep_0", -1)
    near_partial = hidden_and_partial([near])
    next_partial = hidden_and_partial([up, down])
    far_partial = hidden_and_partial([far_up, far_down])

    far_mine, far_sent = far_partial()
    far_total = far_mine + other_core(far_sent).astype(HIGH)
    next_mine, next_sent = next_partial()
    next_total = next_mine + other_core(next_sent).astype(HIGH)
    near_mine, near_sent = near_partial()
    near_total = near_mine + other_core(near_sent).astype(HIGH)
    from_down = give_to(far_total[:half].astype(LOW), "ep_0", 1)
    from_up = give_to(far_total[half:].astype(LOW), "ep_0", -1)
    to_up, to_down = next_total[: 2 * half], next_total[2 * half :]
    to_up = jnp.concatenate([to_up[:half] + from_down.astype(HIGH), to_up[half:]], axis=0)
    to_down = jnp.concatenate([to_down[:half], to_down[half:] + from_up.astype(HIGH)], axis=0)
    below = give_to(to_up.astype(LOW), "ep_0", 1)
    above = give_to(to_down.astype(LOW), "ep_0", -1)
    total = near_total + below.astype(HIGH) + above.astype(HIGH)
    n = total.shape[0] // 8
    cut = [total[i * n : j * n].astype(LOW) for i, j in ((2, 4), (4, 6), (6, 7), (7, 8))]
    return far_sum(near_sum(total[: 2 * n], cut)).astype(LOW)


def solution(mesh):
    torus = Mesh(
        mesh.devices.reshape(mesh.shape["groups"], 4, 16, 2), ("groups", "ep_0", "ep_1", "ep_2")
    )
    placed = (
        P(GROUPS_EP, None),
        P(GROUPS_EP, None),
        P(GROUPS_EP, None),
        P(None, EP),
        P(None, EP),
        P(EP, None),
    )
    return jax.shard_map(layer, mesh=torus, in_specs=placed, out_specs=P(GROUPS_EP, None), check_vma=False)
```

```python
import functools

import jax
import jax.numpy as jnp
from jax import lax
from jax.experimental import pallas as pl
from jax.experimental.pallas import tpu as pltpu
from jax.sharding import Mesh
from jax.sharding import PartitionSpec as P


EXPERTS = 16
LANES = 128
EP = ("ep_0", "ep_1", "ep_2")
GROUPS_EP = ("groups", "ep_0", "ep_1", "ep_2")
FAR = (8, 4, 12)
Z_OFFSETS = (0, 8, 4, 12, 1, 9, 5, 13, 15, 7, 3, 11, 2, 10, 14, 6)
LOW, HIGH = jnp.bfloat16, jnp.float32


def take_from(value, axis, offset):
    count = lax.axis_size(axis)
    return lax.ppermute(value, axis, [((i + offset) % count, i) for i in range(count)])


def give_to(value, axis, offset):
    count = lax.axis_size(axis)
    return lax.ppermute(value, axis, [(i, (i + offset) % count) for i in range(count)])


def other_core(value):
    return give_to(value, "ep_2", 1)


def gate_columns(routes, gates):
    member = routes[:, :, None] == jnp.arange(EXPERTS, dtype=routes.dtype)
    left = jnp.sum(jnp.where(member, gates[:, :, None], 0.0), axis=1)
    parts = []
    for _ in range(3):
        part = lax.reduce_precision(left, 8, 7)
        parts.append(part.astype(LOW))
        left = left - part
    columns = jnp.concatenate(parts, axis=1)
    return jnp.pad(columns, ((0, 0), (0, LANES - columns.shape[1])))


def row_order(tok_rows):
    count = lax.axis_size("ep_1")
    wanted = (lax.axis_index("ep_1") + jnp.array(Z_OFFSETS, jnp.int32)) % count
    wanted = (wanted[:, None] * tok_rows + jnp.arange(tok_rows, dtype=jnp.int32)).reshape(-1)
    return (wanted[:, None] == jnp.arange(count * tok_rows, dtype=jnp.int32)).astype(LOW)


def expert_kernel(blocks, steps, expert_ref, order_ref, *refs):
    row_refs, column_refs = refs[:blocks], refs[blocks : 2 * blocks]
    gate_ref, up_ref, down_ref, mine_ref, other_ref = refs[2 * blocks : 2 * blocks + 5]
    gate_sum, up_sum, hidden_ref, weight_ref = refs[2 * blocks + 5 :]
    step = pl.program_id(0)

    @pl.when(step == 0)
    def _():
        gate_sum[...] = jnp.zeros_like(gate_sum)
        up_sum[...] = jnp.zeros_like(up_sum)

    @pl.when(step < steps)
    def _():
        rows = jnp.concatenate([r[...] for r in row_refs], axis=0)
        gate_sum[...] += jnp.dot(rows, gate_ref[...], preferred_element_type=HIGH)
        up_sum[...] += jnp.dot(rows, up_ref[...], preferred_element_type=HIGH)

    @pl.when(step == steps - 1)
    def _():
        gate_act = gate_sum[...]
        hidden = (gate_act / (1.0 + jnp.exp(-gate_act)) * up_sum[...]).astype(LOW)
        columns = jnp.concatenate([r[...] for r in column_refs], axis=0)
        order = order_ref[...]
        count = order.shape[0]
        index = lax.broadcasted_iota(jnp.int32, (count, LANES), 1)
        mine = (lax.rem(index, EXPERTS) == expert_ref[0]) & (index < 3 * EXPERTS)
        for at in range(0, hidden.shape[0], count):
            moved = jnp.dot(order, hidden[at : at + count], preferred_element_type=HIGH)
            hidden_ref[at : at + count, :] = moved.astype(LOW)
            moved = jnp.dot(order, columns[at : at + count], preferred_element_type=HIGH)
            weight = jnp.sum(jnp.where(mine, moved, 0.0), axis=1, keepdims=True)
            weight_ref[at : at + count, :] = jnp.broadcast_to(weight, (count, LANES))

    @pl.when(step >= steps)
    def _():
        result = jnp.dot(hidden_ref[...], down_ref[...], preferred_element_type=HIGH)
        result = result * weight_ref[:, :1]
        count = mine_ref.shape[0]
        mine_ref[...] = result[:count]
        other_ref[...] = result[count:].astype(LOW)


def expert_of(expert, order, blocks, gate_weight, up_weight, down_weight):
    width, units = gate_weight.shape
    steps = 4
    chunk = width // steps
    rows = sum(block.shape[0] for block in blocks)
    whole = lambda k: (0, 0)
    first = lambda k: jnp.minimum(k, steps - 1)
    second = lambda k: jnp.maximum(k - steps, 0)
    half = pl.BlockSpec((rows // 2, chunk), lambda k: (0, second(k)))
    return pl.pallas_call(
        functools.partial(expert_kernel, len(blocks), steps),
        grid=(2 * steps,),
        in_specs=[
            pl.BlockSpec(memory_space=pltpu.SMEM),
            pl.BlockSpec(order.shape, whole),
            *[pl.BlockSpec((block.shape[0], chunk), lambda k: (0, first(k))) for block in blocks],
            *[pl.BlockSpec((block.shape[0], LANES), lambda k: (0, width // LANES)) for block in blocks],
            pl.BlockSpec((chunk, units), lambda k: (first(k), 0)),
            pl.BlockSpec((chunk, units), lambda k: (first(k), 0)),
            pl.BlockSpec((units, chunk), lambda k: (0, second(k))),
        ],
        out_specs=[half, half],
        out_shape=[jax.ShapeDtypeStruct((rows // 2, width), t) for t in (HIGH, LOW)],
        scratch_shapes=[
            pltpu.VMEM((rows, units), HIGH),
            pltpu.VMEM((rows, units), HIGH),
            pltpu.VMEM((rows, units), LOW),
            pltpu.VMEM((rows, LANES), HIGH),
        ],
        cost_estimate=pl.CostEstimate(
            flops=2 * rows * width * 3 * units,
            bytes_accessed=2 * width * (3 * rows + 3 * units),
            transcendentals=rows * units,
        ),
        name="expert",
    )(expert, order, *blocks, *blocks, gate_weight, up_weight, down_weight)


def near_sum(kept, pieces):
    got = []
    for piece, k in zip(pieces, (1, -1, 2, -2)):
        got.append(give_to(piece, "ep_1", k))
    total = kept + got[0].astype(HIGH) + got[1].astype(HIGH)
    half = got[2].shape[-2]
    top = total[..., :half, :] + got[2].astype(HIGH) + got[3].astype(HIGH)
    return jnp.concatenate([top, total[..., half:, :]], axis=-2)


def far_sum(rows):
    count = rows.shape[-2] // 4
    total = rows[..., :count, :]
    for i, k in enumerate(FAR):
        piece = rows[..., (i + 1) * count : (i + 2) * count, :]
        total = total + give_to(piece.astype(LOW), "ep_1", k).astype(HIGH)
    return total


def layer(tokens, routes, gates, gate_weight, up_weight, down_weight):
    expert = lax.axis_index(EP) // (lax.axis_size(EP) // EXPERTS)
    expert = expert.astype(jnp.int32).reshape(1)
    order = row_order(tokens.shape[0])

    def total_of(blocks):
        with_core = blocks + [other_core(block) for block in blocks]
        mine, sent = expert_of(expert, order, with_core, gate_weight, up_weight, down_weight)
        got = other_core(sent)
        return mine + got.astype(HIGH)

    def moved(value, move, offset):
        return move(value.astype(LOW), "ep_0", offset)

    own = jnp.concatenate([tokens, gate_columns(routes, gates)], axis=1)
    near = lax.all_gather(own, "ep_1", axis=0, tiled=True)
    half = near.shape[0] // 2
    up = moved(near, take_from, 1)
    down = moved(near, take_from, -1)
    far_up = moved(up[:half], take_from, 1)
    far_down = moved(down[half:], take_from, -1)

    near_total = total_of([near])
    next_total = total_of([up, down])
    to_up, to_down = next_total[: 2 * half], next_total[2 * half :]
    below_b = moved(to_up[half:], give_to, 1)
    above_b = moved(to_down[:half], give_to, -1)
    far_total = total_of([far_up, far_down])
    from_below = moved(far_total[:half], give_to, 1)
    from_above = moved(far_total[half:], give_to, -1)
    below_a = moved(to_up[:half] + from_below.astype(HIGH), give_to, 1)
    above_a = moved(to_down[half:] + from_above.astype(HIGH), give_to, -1)
    top = near_total[:half] + above_b.astype(HIGH) + below_a.astype(HIGH)
    bottom = near_total[half:] + below_b.astype(HIGH) + above_a.astype(HIGH)
    total = jnp.concatenate([top, bottom], axis=0)
    n = total.shape[0] // 8
    cut = [total[i * n : j * n].astype(LOW) for i, j in ((2, 4), (4, 6), (6, 7), (7, 8))]
    return far_sum(near_sum(total[: 2 * n], cut)).astype(LOW)


def solution(mesh):
    torus = Mesh(
        mesh.devices.reshape(mesh.shape["groups"], 4, 16, 2), ("groups", "ep_0", "ep_1", "ep_2")
    )
    placed = (
        P(GROUPS_EP, None),
        P(GROUPS_EP, None),
        P(GROUPS_EP, None),
        P(None, EP),
        P(None, EP),
        P(EP, None),
    )
    return jax.shard_map(layer, mesh=torus, in_specs=placed, out_specs=P(GROUPS_EP, None), check_vma=False)
```

```python
import functools

import jax
import jax.numpy as jnp
from jax import lax
from jax.experimental import pallas as pl
from jax.experimental.pallas import tpu as pltpu
from jax.sharding import Mesh
from jax.sharding import PartitionSpec as P


EXPERTS = 16
LANES = 128
STEPS = 4
VMEM_LIMIT = 8 * 2**20
EP = ("ep_0", "ep_1", "ep_2")
GROUPS_EP = ("groups", "ep_0", "ep_1", "ep_2")
FAR = (8, 4, 12)
Z_OFFSETS = (0, 8, 4, 12, 1, 9, 5, 13, 15, 7, 3, 11, 2, 10, 14, 6)
LOW, HIGH = jnp.bfloat16, jnp.float32


def take_from(value, axis, offset):
    count = lax.axis_size(axis)
    return lax.ppermute(value, axis, [((i + offset) % count, i) for i in range(count)])


def give_to(value, axis, offset):
    count = lax.axis_size(axis)
    return lax.ppermute(value, axis, [(i, (i + offset) % count) for i in range(count)])


def other_core(value):
    return give_to(value, "ep_2", 1)


def gate_columns(routes, gates):
    member = routes[:, :, None] == jnp.arange(EXPERTS, dtype=routes.dtype)
    left = jnp.sum(jnp.where(member, gates[:, :, None], 0.0), axis=1)
    parts = []
    for _ in range(3):
        part = lax.reduce_precision(left, 8, 7)
        parts.append(part.astype(LOW))
        left = left - part
    columns = jnp.concatenate(parts, axis=1)
    return jnp.pad(columns, ((0, 0), (0, LANES - columns.shape[1])))


def row_order(tok_rows):
    count = lax.axis_size("ep_1")
    wanted = (lax.axis_index("ep_1") + jnp.array(Z_OFFSETS, jnp.int32)) % count
    wanted = (wanted[:, None] * tok_rows + jnp.arange(tok_rows, dtype=jnp.int32)).reshape(-1)
    return (wanted[:, None] == jnp.arange(count * tok_rows, dtype=jnp.int32)).astype(LOW)


def expert_kernel(blocks, expert_ref, order_ref, *refs):
    row_refs = refs[:blocks]
    gate_ref, up_ref, down_ref, mine_ref, other_ref = refs[blocks : blocks + 5]
    gate_sum, up_sum, hidden_ref, weight_ref = refs[blocks + 5 :]
    width = gate_ref.shape[0]
    chunk = width // STEPS
    gate_sum[...] = jnp.zeros_like(gate_sum)
    up_sum[...] = jnp.zeros_like(up_sum)

    def add(k, carry):
        at = pl.ds(pl.multiple_of(k * chunk, chunk), chunk)
        rows = jnp.concatenate([r[:, at] for r in row_refs], axis=0)
        gate_sum[...] += jnp.dot(rows, gate_ref[at, :], preferred_element_type=HIGH)
        up_sum[...] += jnp.dot(rows, up_ref[at, :], preferred_element_type=HIGH)
        return carry

    lax.fori_loop(0, STEPS, add, 0)
    gate_act = gate_sum[...]
    hidden = (gate_act / (1.0 + jnp.exp(-gate_act)) * up_sum[...]).astype(LOW)
    columns = jnp.concatenate([r[:, width:] for r in row_refs], axis=0)
    order = order_ref[...]
    count = order.shape[0]
    index = lax.broadcasted_iota(jnp.int32, (count, LANES), 1)
    mine = (lax.rem(index, EXPERTS) == expert_ref[0]) & (index < 3 * EXPERTS)
    for at in range(0, hidden.shape[0], count):
        moved = jnp.dot(order, hidden[at : at + count], preferred_element_type=HIGH)
        hidden_ref[at : at + count, :] = moved.astype(LOW)
        moved = jnp.dot(order, columns[at : at + count], preferred_element_type=HIGH)
        weight = jnp.sum(jnp.where(mine, moved, 0.0), axis=1, keepdims=True)
        weight_ref[at : at + count, :] = jnp.broadcast_to(weight, (count, LANES))

    def give(k, carry):
        at = pl.ds(pl.multiple_of(k * chunk, chunk), chunk)
        result = jnp.dot(hidden_ref[...], down_ref[:, at], preferred_element_type=HIGH)
        result = result * weight_ref[:, :1]
        half = mine_ref.shape[0]
        mine_ref[:, at] = result[:half]
        other_ref[:, at] = result[half:].astype(LOW)
        return carry

    lax.fori_loop(0, STEPS, give, 0)


def expert_of(expert, order, blocks, gate_weight, up_weight, down_weight):
    width, units = gate_weight.shape
    rows = sum(block.shape[0] for block in blocks)
    operands = [order, *blocks, gate_weight, up_weight, down_weight]
    operands = [pltpu.with_memory_space_constraint(value, pltpu.VMEM) for value in operands]
    in_vmem = pl.BlockSpec(memory_space=pltpu.VMEM)
    return pl.pallas_call(
        functools.partial(expert_kernel, len(blocks)),
        in_specs=[pl.BlockSpec(memory_space=pltpu.SMEM)] + [in_vmem for _ in operands],
        out_specs=[in_vmem, in_vmem],
        out_shape=[pltpu.VMEM((rows // 2, width), t) for t in (HIGH, LOW)],
        scratch_shapes=[
            pltpu.VMEM((rows, units), HIGH),
            pltpu.VMEM((rows, units), HIGH),
            pltpu.VMEM((rows, units), LOW),
            pltpu.VMEM((rows, LANES), HIGH),
        ],
        compiler_params=pltpu.CompilerParams(vmem_limit_bytes=VMEM_LIMIT),
        cost_estimate=pl.CostEstimate(
            flops=2 * rows * width * 3 * units,
            bytes_accessed=2 * width * (3 * rows + 3 * units),
            transcendentals=rows * units,
        ),
        name="expert",
    )(expert, *operands)


def near_sum(kept, pieces):
    got = []
    for piece, k in zip(pieces, (1, -1, 2, -2)):
        got.append(give_to(piece, "ep_1", k))
    total = kept + got[0].astype(HIGH) + got[1].astype(HIGH)
    half = got[2].shape[-2]
    top = total[..., :half, :] + got[2].astype(HIGH) + got[3].astype(HIGH)
    return jnp.concatenate([top, total[..., half:, :]], axis=-2)


def far_sum(rows):
    count = rows.shape[-2] // 4
    total = rows[..., :count, :]
    for i, k in enumerate(FAR):
        piece = rows[..., (i + 1) * count : (i + 2) * count, :]
        total = total + give_to(piece.astype(LOW), "ep_1", k).astype(HIGH)
    return total


def layer(tokens, routes, gates, gate_weight, up_weight, down_weight):
    expert = lax.axis_index(EP) // (lax.axis_size(EP) // EXPERTS)
    expert = expert.astype(jnp.int32).reshape(1)
    order = row_order(tokens.shape[0])

    def total_of(blocks):
        with_core = blocks + [other_core(block) for block in blocks]
        mine, sent = expert_of(expert, order, with_core, gate_weight, up_weight, down_weight)
        got = other_core(sent)
        return mine + got.astype(HIGH)

    def moved(value, move, offset):
        return move(value.astype(LOW), "ep_0", offset)

    own = jnp.concatenate([tokens, gate_columns(routes, gates)], axis=1)
    near = lax.all_gather(own, "ep_1", axis=0, tiled=True)
    half = near.shape[0] // 2
    up = moved(near, take_from, 1)
    down = moved(near, take_from, -1)
    far_up = moved(up[:half], take_from, 1)
    far_down = moved(down[half:], take_from, -1)

    near_total = total_of([near])
    next_total = total_of([up, down])
    to_up, to_down = next_total[: 2 * half], next_total[2 * half :]
    below_b = moved(to_up[half:], give_to, 1)
    above_b = moved(to_down[:half], give_to, -1)
    far_total = total_of([far_up, far_down])
    from_below = moved(far_total[:half], give_to, 1)
    from_above = moved(far_total[half:], give_to, -1)
    below_a = moved(to_up[:half] + from_below.astype(HIGH), give_to, 1)
    above_a = moved(to_down[half:] + from_above.astype(HIGH), give_to, -1)
    top = near_total[:half] + above_b.astype(HIGH) + below_a.astype(HIGH)
    bottom = near_total[half:] + below_b.astype(HIGH) + above_a.astype(HIGH)
    total = jnp.concatenate([top, bottom], axis=0)
    n = total.shape[0] // 8
    cut = [total[i * n : j * n].astype(LOW) for i, j in ((2, 4), (4, 6), (6, 7), (7, 8))]
    return far_sum(near_sum(total[: 2 * n], cut)).astype(LOW)


def solution(mesh):
    torus = Mesh(
        mesh.devices.reshape(mesh.shape["groups"], 4, 16, 2), ("groups", "ep_0", "ep_1", "ep_2")
    )
    placed = (
        P(GROUPS_EP, None),
        P(GROUPS_EP, None),
        P(GROUPS_EP, None),
        P(None, EP),
        P(None, EP),
        P(EP, None),
    )
    return jax.shard_map(layer, mesh=torus, in_specs=placed, out_specs=P(GROUPS_EP, None), check_vma=False)
```

```python
import functools

import jax
import jax.numpy as jnp
from jax import lax
from jax.experimental import pallas as pl
from jax.experimental.pallas import tpu as pltpu
from jax.sharding import Mesh
from jax.sharding import PartitionSpec as P


EXPERTS = 16
LANES = 128
STEPS = 4
VMEM_LIMIT = 8 * 2**20
EP = ("ep_0", "ep_1", "ep_2")
GROUPS_EP = ("groups", "ep_0", "ep_1", "ep_2")
FAR = (8, 4, 12)
Z_OFFSETS = (0, 8, 4, 12, 1, 9, 5, 13, 15, 7, 3, 11, 2, 10, 14, 6)
LOW, HIGH = jnp.bfloat16, jnp.float32


def take_from(value, axis, offset):
    count = lax.axis_size(axis)
    return lax.ppermute(value, axis, [((i + offset) % count, i) for i in range(count)])


def give_to(value, axis, offset):
    count = lax.axis_size(axis)
    return lax.ppermute(value, axis, [(i, (i + offset) % count) for i in range(count)])


def other_core(value):
    return give_to(value, "ep_2", 1)


def gate_columns(routes, gates):
    member = routes[:, :, None] == jnp.arange(EXPERTS, dtype=routes.dtype)
    left = jnp.sum(jnp.where(member, gates[:, :, None], 0.0), axis=1)
    parts = []
    for _ in range(3):
        part = lax.reduce_precision(left, 8, 7)
        parts.append(part.astype(LOW))
        left = left - part
    columns = jnp.concatenate(parts, axis=1)
    return jnp.pad(columns, ((0, 0), (0, LANES - columns.shape[1])))


def row_order(tok_rows):
    count = lax.axis_size("ep_1")
    wanted = (lax.axis_index("ep_1") + jnp.array(Z_OFFSETS, jnp.int32)) % count
    wanted = (wanted[:, None] * tok_rows + jnp.arange(tok_rows, dtype=jnp.int32)).reshape(-1)
    return (wanted[:, None] == jnp.arange(count * tok_rows, dtype=jnp.int32)).astype(LOW)


def expert_kernel(blocks, expert_ref, order_ref, *refs):
    row_refs = refs[:blocks]
    gate_ref, up_ref, down_ref, mine_ref, other_ref = refs[blocks : blocks + 5]
    gate_sum, up_sum, hidden_ref, weight_ref = refs[blocks + 5 :]
    width = gate_ref.shape[0]
    chunk = width // STEPS
    gate_sum[...] = jnp.zeros_like(gate_sum)
    up_sum[...] = jnp.zeros_like(up_sum)

    def add(k, carry):
        at = pl.ds(pl.multiple_of(k * chunk, chunk), chunk)
        rows = jnp.concatenate([r[:, at] for r in row_refs], axis=0)
        gate_sum[...] += jnp.dot(rows, gate_ref[at, :], preferred_element_type=HIGH)
        up_sum[...] += jnp.dot(rows, up_ref[at, :], preferred_element_type=HIGH)
        return carry

    lax.fori_loop(0, STEPS, add, 0)
    gate_act = gate_sum[...]
    hidden = (gate_act / (1.0 + jnp.exp(-gate_act)) * up_sum[...]).astype(LOW)
    columns = jnp.concatenate([r[:, width:] for r in row_refs], axis=0)
    order = order_ref[...]
    count = order.shape[0]
    index = lax.broadcasted_iota(jnp.int32, (count, LANES), 1)
    mine = (lax.rem(index, EXPERTS) == expert_ref[0]) & (index < 3 * EXPERTS)
    for at in range(0, hidden.shape[0], count):
        moved = jnp.dot(order, hidden[at : at + count], preferred_element_type=HIGH)
        hidden_ref[at : at + count, :] = moved.astype(LOW)
        moved = jnp.dot(order, columns[at : at + count], preferred_element_type=HIGH)
        weight = jnp.sum(jnp.where(mine, moved, 0.0), axis=1, keepdims=True)
        weight_ref[at : at + count, :] = jnp.broadcast_to(weight, (count, LANES))

    def give(k, carry):
        at = pl.ds(pl.multiple_of(k * chunk, chunk), chunk)
        result = jnp.dot(hidden_ref[...], down_ref[:, at], preferred_element_type=HIGH)
        result = result * weight_ref[:, :1]
        half = mine_ref.shape[0]
        mine_ref[:, at] = result[:half]
        other_ref[:, at] = result[half:].astype(LOW)
        return carry

    lax.fori_loop(0, STEPS, give, 0)


def expert_of(expert, order, blocks, gate_weight, up_weight, down_weight):
    width, units = gate_weight.shape
    rows = sum(block.shape[0] for block in blocks)
    operands = [order, *blocks, gate_weight, up_weight, down_weight]
    operands = [pltpu.with_memory_space_constraint(value, pltpu.VMEM) for value in operands]
    in_vmem = pl.BlockSpec(memory_space=pltpu.VMEM)
    return pl.pallas_call(
        functools.partial(expert_kernel, len(blocks)),
        in_specs=[pl.BlockSpec(memory_space=pltpu.SMEM)] + [in_vmem for _ in operands],
        out_specs=[in_vmem, in_vmem],
        out_shape=[pltpu.VMEM((rows // 2, width), t) for t in (HIGH, LOW)],
        scratch_shapes=[
            pltpu.VMEM((rows, units), HIGH),
            pltpu.VMEM((rows, units), HIGH),
            pltpu.VMEM((rows, units), LOW),
            pltpu.VMEM((rows, LANES), HIGH),
        ],
        compiler_params=pltpu.CompilerParams(vmem_limit_bytes=VMEM_LIMIT),
        cost_estimate=pl.CostEstimate(
            flops=2 * rows * width * 3 * units,
            bytes_accessed=2 * width * (3 * rows + 3 * units),
            transcendentals=rows * units,
        ),
        name="expert",
    )(expert, *operands)


def copied(value):
    def copy_kernel(from_ref, to_ref):
        to_ref[...] = from_ref[...]

    in_vmem = pl.BlockSpec(memory_space=pltpu.VMEM)
    return pl.pallas_call(
        copy_kernel,
        in_specs=[in_vmem],
        out_specs=in_vmem,
        out_shape=pltpu.VMEM(value.shape, value.dtype),
        compiler_params=pltpu.CompilerParams(vmem_limit_bytes=2**20),
        name="copied",
    )(pltpu.with_memory_space_constraint(value, pltpu.VMEM))


def near_sum(kept, pieces):
    got = []
    for piece, k in zip(pieces, (1, -1, 2, -2)):
        got.append(give_to(piece, "ep_1", k))
    total = kept + got[0].astype(HIGH) + got[1].astype(HIGH)
    half = got[2].shape[-2]
    top = total[..., :half, :] + got[2].astype(HIGH) + got[3].astype(HIGH)
    return jnp.concatenate([top, total[..., half:, :]], axis=-2)


def far_sum(rows):
    count = rows.shape[-2] // 4
    total = rows[..., :count, :]
    for i, k in enumerate(FAR):
        piece = rows[..., (i + 1) * count : (i + 2) * count, :]
        total = total + give_to(piece.astype(LOW), "ep_1", k).astype(HIGH)
    return total


def layer(tokens, routes, gates, gate_weight, up_weight, down_weight):
    expert = lax.axis_index(EP) // (lax.axis_size(EP) // EXPERTS)
    expert = expert.astype(jnp.int32).reshape(1)
    order_near = row_order(tokens.shape[0])
    order_next = copied(order_near)

    def total_of(blocks, order):
        with_core = blocks + [other_core(block) for block in blocks]
        mine, sent = expert_of(expert, order, with_core, gate_weight, up_weight, down_weight)
        got = other_core(sent)
        return mine + got.astype(HIGH)

    def moved(value, move, offset):
        return move(value.astype(LOW), "ep_0", offset)

    own = jnp.concatenate([tokens, gate_columns(routes, gates)], axis=1)
    near = lax.all_gather(own, "ep_1", axis=0, tiled=True)
    half = near.shape[0] // 2
    up_a = moved(near[:half], take_from, 1)
    down_b = moved(near[half:], take_from, -1)
    up_b = moved(near[half:], take_from, 1)
    down_a = moved(near[:half], take_from, -1)
    far_up = moved(up_a, take_from, 1)
    far_down = moved(down_b, take_from, -1)

    near_total = total_of([near], order_near)
    next_total = total_of([up_a, up_b, down_a, down_b], order_next)
    to_up, to_down = next_total[: 2 * half], next_total[2 * half :]
    below_b = moved(to_up[half:], give_to, 1)
    above_b = moved(to_down[:half], give_to, -1)
    far_total = total_of([far_up, far_down], order_next)
    from_below = moved(far_total[:half], give_to, 1)
    from_above = moved(far_total[half:], give_to, -1)
    below_a = moved(to_up[:half] + from_below.astype(HIGH), give_to, 1)
    above_a = moved(to_down[half:] + from_above.astype(HIGH), give_to, -1)
    top = near_total[:half] + above_b.astype(HIGH) + below_a.astype(HIGH)
    bottom = near_total[half:] + below_b.astype(HIGH) + above_a.astype(HIGH)
    total = jnp.concatenate([top, bottom], axis=0)
    n = total.shape[0] // 8
    cut = [total[i * n : j * n].astype(LOW) for i, j in ((2, 4), (4, 6), (6, 7), (7, 8))]
    return far_sum(near_sum(total[: 2 * n], cut)).astype(LOW)


def solution(mesh):
    torus = Mesh(
        mesh.devices.reshape(mesh.shape["groups"], 4, 16, 2), ("groups", "ep_0", "ep_1", "ep_2")
    )
    placed = (
        P(GROUPS_EP, None),
        P(GROUPS_EP, None),
        P(GROUPS_EP, None),
        P(None, EP),
        P(None, EP),
        P(EP, None),
    )
    return jax.shard_map(
        layer, mesh=torus, in_specs=placed, out_specs=P(GROUPS_EP, None), check_vma=False
    )
```

```python
import functools

import jax
import jax.numpy as jnp
from jax import lax
from jax.experimental import pallas as pl
from jax.experimental.pallas import tpu as pltpu
from jax.sharding import Mesh
from jax.sharding import PartitionSpec as P


EXPERTS = 16
LANES = 128
STEPS = 4
VMEM_LIMIT = 8 * 2**20
EP = ("ep_0", "ep_1", "ep_2")
GROUPS_EP = ("groups", "ep_0", "ep_1", "ep_2")
FAR = (8, 4, 12)
Z_OFFSETS = (0, 8, 4, 12, 1, 9, 5, 13, 15, 7, 3, 11, 2, 10, 14, 6)
LOW, HIGH = jnp.bfloat16, jnp.float32


def take_from(value, axis, offset):
    count = lax.axis_size(axis)
    return lax.ppermute(value, axis, [((i + offset) % count, i) for i in range(count)])


def give_to(value, axis, offset):
    count = lax.axis_size(axis)
    return lax.ppermute(value, axis, [(i, (i + offset) % count) for i in range(count)])


def other_core(value):
    return give_to(value, "ep_2", 1)


def gate_columns(routes, gates):
    member = routes[:, :, None] == jnp.arange(EXPERTS, dtype=routes.dtype)
    left = jnp.sum(jnp.where(member, gates[:, :, None], 0.0), axis=1)
    parts = []
    for _ in range(3):
        part = lax.reduce_precision(left, 8, 7)
        parts.append(part.astype(LOW))
        left = left - part
    columns = jnp.concatenate(parts, axis=1)
    return jnp.pad(columns, ((0, 0), (0, LANES - columns.shape[1])))


def row_order(tok_rows):
    count = lax.axis_size("ep_1")
    wanted = (lax.axis_index("ep_1") + jnp.array(Z_OFFSETS, jnp.int32)) % count
    wanted = (wanted[:, None] * tok_rows + jnp.arange(tok_rows, dtype=jnp.int32)).reshape(-1)
    return (wanted[:, None] == jnp.arange(count * tok_rows, dtype=jnp.int32)).astype(LOW)


def expert_kernel(blocks, expert_ref, *refs):
    row_refs = refs[:blocks]
    gate_ref, up_ref, down_ref, mine_ref, other_ref = refs[blocks : blocks + 5]
    gate_sum, up_sum, hidden_ref, weight_ref = refs[blocks + 5 :]
    width = gate_ref.shape[0]
    chunk = width // STEPS
    gate_sum[...] = jnp.zeros_like(gate_sum)
    up_sum[...] = jnp.zeros_like(up_sum)

    def add(k, carry):
        at = pl.ds(pl.multiple_of(k * chunk, chunk), chunk)
        rows = jnp.concatenate([r[:, at] for r in row_refs], axis=0)
        gate_sum[...] += jnp.dot(rows, gate_ref[at, :], preferred_element_type=HIGH)
        up_sum[...] += jnp.dot(rows, up_ref[at, :], preferred_element_type=HIGH)
        return carry

    lax.fori_loop(0, STEPS, add, 0)
    gate_act = gate_sum[...]
    hidden = (gate_act / (1.0 + jnp.exp(-gate_act)) * up_sum[...]).astype(LOW)
    columns = jnp.concatenate([r[:, width:] for r in row_refs], axis=0)
    hidden_ref[...] = hidden
    index = lax.broadcasted_iota(jnp.int32, columns.shape, 1)
    mine = (lax.rem(index, EXPERTS) == expert_ref[0]) & (index < 3 * EXPERTS)
    weight = jnp.sum(jnp.where(mine, columns.astype(HIGH), 0.0), axis=1, keepdims=True)
    weight_ref[...] = jnp.broadcast_to(weight, weight_ref.shape)

    def give(k, carry):
        at = pl.ds(pl.multiple_of(k * chunk, chunk), chunk)
        result = jnp.dot(hidden_ref[...], down_ref[:, at], preferred_element_type=HIGH)
        result = result * weight_ref[:, :1]
        half = mine_ref.shape[0]
        mine_ref[:, at] = result[:half]
        other_ref[:, at] = result[half:].astype(LOW)
        return carry

    lax.fori_loop(0, STEPS, give, 0)


def expert_of(expert, blocks, gate_weight, up_weight, down_weight):
    width, units = gate_weight.shape
    rows = sum(block.shape[0] for block in blocks)
    operands = [*blocks, gate_weight, up_weight, down_weight]
    operands = [pltpu.with_memory_space_constraint(value, pltpu.VMEM) for value in operands]
    in_vmem = pl.BlockSpec(memory_space=pltpu.VMEM)
    return pl.pallas_call(
        functools.partial(expert_kernel, len(blocks)),
        in_specs=[pl.BlockSpec(memory_space=pltpu.SMEM)] + [in_vmem for _ in operands],
        out_specs=[in_vmem, in_vmem],
        out_shape=[pltpu.VMEM((rows // 2, width), t) for t in (HIGH, LOW)],
        scratch_shapes=[
            pltpu.VMEM((rows, units), HIGH),
            pltpu.VMEM((rows, units), HIGH),
            pltpu.VMEM((rows, units), LOW),
            pltpu.VMEM((rows, LANES), HIGH),
        ],
        compiler_params=pltpu.CompilerParams(vmem_limit_bytes=VMEM_LIMIT),
        cost_estimate=pl.CostEstimate(
            flops=2 * rows * width * 3 * units,
            bytes_accessed=2 * width * (3 * rows + 3 * units),
            transcendentals=rows * units,
        ),
        name="expert",
    )(expert, *operands)


def copied(value):
    def copy_kernel(from_ref, to_ref):
        to_ref[...] = from_ref[...]

    in_vmem = pl.BlockSpec(memory_space=pltpu.VMEM)
    return pl.pallas_call(
        copy_kernel,
        in_specs=[in_vmem],
        out_specs=in_vmem,
        out_shape=pltpu.VMEM(value.shape, value.dtype),
        compiler_params=pltpu.CompilerParams(vmem_limit_bytes=2**20),
        name="copied",
    )(pltpu.with_memory_space_constraint(value, pltpu.VMEM))


def near_sum(kept, pieces):
    got = []
    for piece, k in zip(pieces, (1, -1, 2, -2)):
        got.append(give_to(piece, "ep_1", k))
    total = kept + got[0].astype(HIGH) + got[1].astype(HIGH)
    half = got[2].shape[-2]
    top = total[..., :half, :] + got[2].astype(HIGH) + got[3].astype(HIGH)
    return jnp.concatenate([top, total[..., half:, :]], axis=-2)


def far_sum(rows):
    count = rows.shape[-2] // 4
    total = rows[..., :count, :]
    for i, k in enumerate(FAR):
        piece = rows[..., (i + 1) * count : (i + 2) * count, :]
        total = total + give_to(piece.astype(LOW), "ep_1", k).astype(HIGH)
    return total


def layer(tokens, routes, gates, gate_weight, up_weight, down_weight):
    expert = lax.axis_index(EP) // (lax.axis_size(EP) // EXPERTS)
    expert = expert.astype(jnp.int32).reshape(1)
    order = copied(row_order(tokens.shape[0]))

    def total_of(blocks):
        with_core = blocks + [other_core(block) for block in blocks]
        mine, sent = expert_of(expert, with_core, gate_weight, up_weight, down_weight)
        got = other_core(sent)
        return mine + got.astype(HIGH)

    def moved(value, move, offset):
        return move(value.astype(LOW), "ep_0", offset)

    own = jnp.concatenate([tokens, gate_columns(routes, gates)], axis=1)
    near = lax.optimization_barrier(lax.all_gather(own, "ep_1", axis=0, tiled=True))
    half = near.shape[0] // 2
    up_a = moved(near[:half], take_from, 1)
    down_b = moved(near[half:], take_from, -1)
    up_b = moved(near[half:], take_from, 1)
    down_a = moved(near[:half], take_from, -1)
    far_up = moved(up_a, take_from, 1)
    far_down = moved(down_b, take_from, -1)

    near_total = total_of([near])
    total_b = total_of([up_b, down_a])
    below_b = moved(total_b[:half], give_to, 1)
    above_b = moved(total_b[half:], give_to, -1)
    far_total = total_of([far_up, far_down])
    from_below = moved(far_total[:half], give_to, 1)
    from_above = moved(far_total[half:], give_to, -1)
    total_a = total_of([up_a, down_b])
    below_a = moved(total_a[:half] + from_below.astype(HIGH), give_to, 1)
    above_a = moved(total_a[half:] + from_above.astype(HIGH), give_to, -1)
    top = near_total[:half] + above_b.astype(HIGH) + below_a.astype(HIGH)
    bottom = near_total[half:] + below_b.astype(HIGH) + above_a.astype(HIGH)
    total = jnp.concatenate([top, bottom], axis=0).astype(LOW)
    total = jnp.dot(order, total, preferred_element_type=HIGH)
    n = total.shape[0] // 8
    cut = [total[i * n : j * n].astype(LOW) for i, j in ((2, 4), (4, 6), (6, 7), (7, 8))]
    return far_sum(near_sum(total[: 2 * n], cut)).astype(LOW)


def solution(mesh):
    torus = Mesh(
        mesh.devices.reshape(mesh.shape["groups"], 4, 16, 2), ("groups", "ep_0", "ep_1", "ep_2")
    )
    placed = (
        P(GROUPS_EP, None),
        P(GROUPS_EP, None),
        P(GROUPS_EP, None),
        P(None, EP),
        P(None, EP),
        P(EP, None),
    )
    return jax.shard_map(
        layer, mesh=torus, in_specs=placed, out_specs=P(GROUPS_EP, None), check_vma=False
    )
```

```python
import functools

import jax
import jax.numpy as jnp
from jax import lax
from jax.experimental import pallas as pl
from jax.experimental.pallas import tpu as pltpu
from jax.sharding import Mesh
from jax.sharding import PartitionSpec as P


EXPERTS = 16
LANES = 128
STEPS = 4
VMEM_LIMIT = 8 * 2**20
EP = ("ep_0", "ep_1", "ep_2")
GROUPS_EP = ("groups", "ep_0", "ep_1", "ep_2")
FAR = (8, 4, 12)
Z_OFFSETS = (0, 8, 4, 12, 1, 9, 5, 13, 15, 7, 3, 11, 2, 10, 14, 6)
LOW, HIGH = jnp.bfloat16, jnp.float32


def take_from(value, axis, offset):
    count = lax.axis_size(axis)
    return lax.ppermute(value, axis, [((i + offset) % count, i) for i in range(count)])


def give_to(value, axis, offset):
    count = lax.axis_size(axis)
    return lax.ppermute(value, axis, [(i, (i + offset) % count) for i in range(count)])


def other_core(value):
    return give_to(value, "ep_2", 1)


def gate_columns(routes, gates):
    member = routes[:, :, None] == jnp.arange(EXPERTS, dtype=routes.dtype)
    left = jnp.sum(jnp.where(member, gates[:, :, None], 0.0), axis=1)
    parts = []
    for _ in range(3):
        part = lax.reduce_precision(left, 8, 7)
        parts.append(part.astype(LOW))
        left = left - part
    columns = jnp.concatenate(parts, axis=1)
    return jnp.pad(columns, ((0, 0), (0, LANES - columns.shape[1])))


def row_order(tok_rows):
    count = lax.axis_size("ep_1")
    wanted = (lax.axis_index("ep_1") + jnp.array(Z_OFFSETS, jnp.int32)) % count
    wanted = (wanted[:, None] * tok_rows + jnp.arange(tok_rows, dtype=jnp.int32)).reshape(-1)
    return (wanted[:, None] == jnp.arange(count * tok_rows, dtype=jnp.int32)).astype(LOW)


def expert_kernel(blocks, expert_ref, *refs):
    row_refs = refs[:blocks]
    gate_ref, up_ref, down_ref, mine_ref, other_ref = refs[blocks : blocks + 5]
    gate_sum, up_sum, hidden_ref, weight_ref = refs[blocks + 5 :]
    width = gate_ref.shape[0]
    chunk = width // STEPS
    gate_sum[...] = jnp.zeros_like(gate_sum)
    up_sum[...] = jnp.zeros_like(up_sum)

    def add(k, carry):
        at = pl.ds(pl.multiple_of(k * chunk, chunk), chunk)
        rows = jnp.concatenate([r[:, at] for r in row_refs], axis=0)
        gate_sum[...] += jnp.dot(rows, gate_ref[at, :], preferred_element_type=HIGH)
        up_sum[...] += jnp.dot(rows, up_ref[at, :], preferred_element_type=HIGH)
        return carry

    lax.fori_loop(0, STEPS, add, 0)
    gate_act = gate_sum[...]
    hidden = (gate_act / (1.0 + jnp.exp(-gate_act)) * up_sum[...]).astype(LOW)
    columns = jnp.concatenate([r[:, width:] for r in row_refs], axis=0)
    hidden_ref[...] = hidden
    index = lax.broadcasted_iota(jnp.int32, columns.shape, 1)
    mine = (lax.rem(index, EXPERTS) == expert_ref[0]) & (index < 3 * EXPERTS)
    weight = jnp.sum(jnp.where(mine, columns.astype(HIGH), 0.0), axis=1, keepdims=True)
    weight_ref[...] = jnp.broadcast_to(weight, weight_ref.shape)

    def give(k, carry):
        at = pl.ds(pl.multiple_of(k * chunk, chunk), chunk)
        result = jnp.dot(hidden_ref[...], down_ref[:, at], preferred_element_type=HIGH)
        result = result * weight_ref[:, :1]
        half = mine_ref.shape[0]
        mine_ref[:, at] = result[:half]
        other_ref[:, at] = result[half:].astype(LOW)
        return carry

    lax.fori_loop(0, STEPS, give, 0)


def expert_of(expert, blocks, gate_weight, up_weight, down_weight):
    width, units = gate_weight.shape
    rows = sum(block.shape[0] for block in blocks)
    operands = [*blocks, gate_weight, up_weight, down_weight]
    operands = [pltpu.with_memory_space_constraint(value, pltpu.VMEM) for value in operands]
    in_vmem = pl.BlockSpec(memory_space=pltpu.VMEM)
    return pl.pallas_call(
        functools.partial(expert_kernel, len(blocks)),
        in_specs=[pl.BlockSpec(memory_space=pltpu.SMEM)] + [in_vmem for _ in operands],
        out_specs=[in_vmem, in_vmem],
        out_shape=[pltpu.VMEM((rows // 2, width), t) for t in (HIGH, LOW)],
        scratch_shapes=[
            pltpu.VMEM((rows, units), HIGH),
            pltpu.VMEM((rows, units), HIGH),
            pltpu.VMEM((rows, units), LOW),
            pltpu.VMEM((rows, LANES), HIGH),
        ],
        compiler_params=pltpu.CompilerParams(vmem_limit_bytes=VMEM_LIMIT),
        cost_estimate=pl.CostEstimate(
            flops=2 * rows * width * 3 * units,
            bytes_accessed=2 * width * (3 * rows + 3 * units),
            transcendentals=rows * units,
        ),
        name="expert",
    )(expert, *operands)


def copied(value):
    def copy_kernel(from_ref, to_ref):
        to_ref[...] = from_ref[...]

    in_vmem = pl.BlockSpec(memory_space=pltpu.VMEM)
    return pl.pallas_call(
        copy_kernel,
        in_specs=[in_vmem],
        out_specs=in_vmem,
        out_shape=pltpu.VMEM(value.shape, value.dtype),
        compiler_params=pltpu.CompilerParams(vmem_limit_bytes=2**20),
        name="copied",
    )(pltpu.with_memory_space_constraint(value, pltpu.VMEM))


def sum_along_z(rows):
    def received(piece, offset):
        return give_to(piece.astype(LOW), "ep_1", offset).astype(HIGH)

    n = rows.shape[0] // 16
    plus = received(rows[4 * n : 8 * n], 1)
    minus = received(rows[8 * n : 12 * n], -1)
    plus_two = received(rows[12 * n : 14 * n], 2)
    minus_two = received(rows[14 * n :], -2)
    near = rows[: 4 * n] + plus + minus
    pieces = near[2 * n : 3 * n].astype(LOW), near[3 * n :].astype(LOW), near[: 2 * n]
    low_b, low_c, top = lax.optimization_barrier(pieces)
    total = received(low_b, FAR[1]) + received(low_c, FAR[2])
    top = copied(top)
    top = top + plus_two + minus_two
    return top[:n] + received(top[n:], FAR[0]) + total


def layer(tokens, routes, gates, gate_weight, up_weight, down_weight):
    expert = lax.axis_index(EP) // (lax.axis_size(EP) // EXPERTS)
    expert = expert.astype(jnp.int32).reshape(1)
    order = copied(row_order(tokens.shape[0]))

    def total_of(blocks):
        with_core = blocks + [other_core(block) for block in blocks]
        mine, sent = expert_of(expert, with_core, gate_weight, up_weight, down_weight)
        got = other_core(sent)
        return mine + got.astype(HIGH)

    def moved(value, move, offset):
        return move(value.astype(LOW), "ep_0", offset)

    own = jnp.concatenate([tokens, gate_columns(routes, gates)], axis=1)
    near = lax.optimization_barrier(lax.all_gather(own, "ep_1", axis=0, tiled=True))
    half = near.shape[0] // 2
    up_a = moved(near[:half], take_from, 1)
    down_b = moved(near[half:], take_from, -1)
    up_b = moved(near[half:], take_from, 1)
    down_a = moved(near[:half], take_from, -1)
    far_up = moved(up_a, take_from, 1)
    far_down = moved(down_b, take_from, -1)

    near_total = total_of([near])
    total_b = total_of([up_b, down_a])
    below_b = moved(total_b[:half], give_to, 1)
    above_b = moved(total_b[half:], give_to, -1)
    far_total = total_of([far_up, far_down])
    from_below = moved(far_total[:half], give_to, 1)
    from_above = moved(far_total[half:], give_to, -1)
    total_a = total_of([up_a, down_b])
    below_a = moved(total_a[:half] + from_below.astype(HIGH), give_to, 1)
    above_a = moved(total_a[half:] + from_above.astype(HIGH), give_to, -1)
    top = near_total[:half] + above_b.astype(HIGH) + below_a.astype(HIGH)
    bottom = near_total[half:] + below_b.astype(HIGH) + above_a.astype(HIGH)
    total = jnp.concatenate([top, bottom], axis=0).astype(LOW)
    total = jnp.dot(order, total, preferred_element_type=HIGH)
    return sum_along_z(total).astype(LOW)


def solution(mesh):
    torus = Mesh(
        mesh.devices.reshape(mesh.shape["groups"], 4, 16, 2), ("groups", "ep_0", "ep_1", "ep_2")
    )
    placed = (
        P(GROUPS_EP, None),
        P(GROUPS_EP, None),
        P(GROUPS_EP, None),
        P(None, EP),
        P(None, EP),
        P(EP, None),
    )
    return jax.shard_map(layer, mesh=torus, in_specs=placed, out_specs=P(GROUPS_EP, None), check_vma=False)
```

```python
import functools

import jax
import jax.numpy as jnp
from jax import lax
from jax.experimental import pallas as pl
from jax.experimental.pallas import tpu as pltpu
from jax.sharding import Mesh
from jax.sharding import PartitionSpec as P


EXPERTS = 16
LANES = 128
STEPS = 4
VMEM_LIMIT = 8 * 2**20
EP = ("ep_0", "ep_1", "ep_2")
GROUPS_EP = ("groups", "ep_0", "ep_1", "ep_2")
Z_OFFSETS = (4, 0, 12, 8, 5, 1, 13, 9, 3, 15, 11, 7, 6, 2, 14, 10)
LOW, HIGH = jnp.bfloat16, jnp.float32


def take_from(value, axis, offset):
    count = lax.axis_size(axis)
    return lax.ppermute(value, axis, [((i + offset) % count, i) for i in range(count)])


def give_to(value, axis, offset):
    count = lax.axis_size(axis)
    return lax.ppermute(value, axis, [(i, (i + offset) % count) for i in range(count)])


def other_core(value):
    return give_to(value, "ep_2", 1)


def gate_columns(routes, gates):
    member = routes[:, :, None] == jnp.arange(EXPERTS, dtype=routes.dtype)
    left = jnp.sum(jnp.where(member, gates[:, :, None], 0.0), axis=1)
    parts = []
    for _ in range(3):
        part = lax.reduce_precision(left, 8, 7)
        parts.append(part.astype(LOW))
        left = left - part
    columns = jnp.concatenate(parts, axis=1)
    return jnp.pad(columns, ((0, 0), (0, LANES - columns.shape[1])))


def row_order(tok_rows):
    count = lax.axis_size("ep_1")
    wanted = (lax.axis_index("ep_1") + jnp.array(Z_OFFSETS, jnp.int32)) % count
    wanted = (wanted[:, None] * tok_rows + jnp.arange(tok_rows, dtype=jnp.int32)).reshape(-1)
    return (wanted[:, None] == jnp.arange(count * tok_rows, dtype=jnp.int32)).astype(LOW)


def expert_kernel(blocks, expert_ref, *refs):
    row_refs = refs[:blocks]
    gate_ref, up_ref, down_ref, mine_ref, other_ref = refs[blocks : blocks + 5]
    gate_sum, up_sum, hidden_ref, weight_ref = refs[blocks + 5 :]
    width = gate_ref.shape[0]
    chunk = width // STEPS
    gate_sum[...] = jnp.zeros_like(gate_sum)
    up_sum[...] = jnp.zeros_like(up_sum)

    def add(k, carry):
        at = pl.ds(pl.multiple_of(k * chunk, chunk), chunk)
        rows = jnp.concatenate([r[:, at] for r in row_refs], axis=0)
        gate_sum[...] += jnp.dot(rows, gate_ref[at, :], preferred_element_type=HIGH)
        up_sum[...] += jnp.dot(rows, up_ref[at, :], preferred_element_type=HIGH)
        return carry

    lax.fori_loop(0, STEPS, add, 0)
    gate_act = gate_sum[...]
    hidden = (gate_act / (1.0 + jnp.exp(-gate_act)) * up_sum[...]).astype(LOW)
    columns = jnp.concatenate([r[:, width:] for r in row_refs], axis=0)
    hidden_ref[...] = hidden
    index = lax.broadcasted_iota(jnp.int32, columns.shape, 1)
    mine = (lax.rem(index, EXPERTS) == expert_ref[0]) & (index < 3 * EXPERTS)
    weight = jnp.sum(jnp.where(mine, columns.astype(HIGH), 0.0), axis=1, keepdims=True)
    weight_ref[...] = jnp.broadcast_to(weight, weight_ref.shape)

    def give(k, carry):
        at = pl.ds(pl.multiple_of(k * chunk, chunk), chunk)
        result = jnp.dot(hidden_ref[...], down_ref[:, at], preferred_element_type=HIGH)
        result = result * weight_ref[:, :1]
        half = mine_ref.shape[0]
        mine_ref[:, at] = result[:half]
        other_ref[:, at] = result[half:].astype(LOW)
        return carry

    lax.fori_loop(0, STEPS, give, 0)


def expert_of(expert, blocks, gate_weight, up_weight, down_weight):
    width, units = gate_weight.shape
    rows = sum(block.shape[0] for block in blocks)
    operands = [*blocks, gate_weight, up_weight, down_weight]
    operands = [pltpu.with_memory_space_constraint(value, pltpu.VMEM) for value in operands]
    in_vmem = pl.BlockSpec(memory_space=pltpu.VMEM)
    return pl.pallas_call(
        functools.partial(expert_kernel, len(blocks)),
        in_specs=[pl.BlockSpec(memory_space=pltpu.SMEM)] + [in_vmem for _ in operands],
        out_specs=[in_vmem, in_vmem],
        out_shape=[pltpu.VMEM((rows // 2, width), t) for t in (HIGH, LOW)],
        scratch_shapes=[
            pltpu.VMEM((rows, units), HIGH),
            pltpu.VMEM((rows, units), HIGH),
            pltpu.VMEM((rows, units), LOW),
            pltpu.VMEM((rows, LANES), HIGH),
        ],
        compiler_params=pltpu.CompilerParams(vmem_limit_bytes=VMEM_LIMIT),
        cost_estimate=pl.CostEstimate(
            flops=2 * rows * width * 3 * units,
            bytes_accessed=2 * width * (3 * rows + 3 * units),
            transcendentals=rows * units,
        ),
        name="expert",
    )(expert, *operands)


def copied(value):
    def copy_kernel(from_ref, to_ref):
        to_ref[...] = from_ref[...]

    in_vmem = pl.BlockSpec(memory_space=pltpu.VMEM)
    return pl.pallas_call(
        copy_kernel,
        in_specs=[in_vmem],
        out_specs=in_vmem,
        out_shape=pltpu.VMEM(value.shape, value.dtype),
        compiler_params=pltpu.CompilerParams(vmem_limit_bytes=2**20),
        name="copied",
    )(pltpu.with_memory_space_constraint(value, pltpu.VMEM))


def sum_along_z(rows):
    def received(piece, offset):
        return give_to(piece.astype(LOW), "ep_1", offset).astype(HIGH)

    n = rows.shape[0] // 16
    plus = received(rows[4 * n : 8 * n], 1)
    minus = received(rows[8 * n : 12 * n], -1)
    plus_two = received(rows[12 * n : 14 * n], 2)
    minus_two = received(rows[14 * n :], -2)
    near = rows[: 4 * n] + plus + minus
    far_a, near = lax.optimization_barrier((near[3 * n :].astype(LOW), near))
    far_a = received(far_a, 8)
    near = copied(near)
    far_b = received(near[:n] + plus_two[:n], 4)
    far_c = received(near[2 * n : 3 * n] + minus_two[n:], 12)
    return near[n : 2 * n] + plus_two[n:] + minus_two[:n] + far_a + far_b + far_c


def layer(tokens, routes, gates, gate_weight, up_weight, down_weight):
    expert = lax.axis_index(EP) // (lax.axis_size(EP) // EXPERTS)
    expert = expert.astype(jnp.int32).reshape(1)
    order = copied(row_order(tokens.shape[0]))

    def total_of(blocks):
        with_core = blocks + [other_core(block) for block in blocks]
        mine, sent = expert_of(expert, with_core, gate_weight, up_weight, down_weight)
        got = other_core(sent)
        return mine + got.astype(HIGH)

    def moved(value, move, offset):
        return move(value.astype(LOW), "ep_0", offset)

    own = jnp.concatenate([tokens, gate_columns(routes, gates)], axis=1)
    near = lax.optimization_barrier(lax.all_gather(own, "ep_1", axis=0, tiled=True))
    half = near.shape[0] // 2
    up_a = moved(near[:half], take_from, 1)
    down_b = moved(near[half:], take_from, -1)
    up_b = moved(near[half:], take_from, 1)
    down_a = moved(near[:half], take_from, -1)
    far_up = moved(up_a, take_from, 1)
    far_down = moved(down_b, take_from, -1)

    near_total = total_of([near])
    total_b = total_of([up_b, down_a])
    below_b = moved(total_b[:half], give_to, 1)
    above_b = moved(total_b[half:], give_to, -1)
    far_total = total_of([far_up, far_down])
    from_below = moved(far_total[:half], give_to, 1)
    from_above = moved(far_total[half:], give_to, -1)
    total_a = total_of([up_a, down_b])
    below_a = moved(total_a[:half] + from_below.astype(HIGH), give_to, 1)
    above_a = moved(total_a[half:] + from_above.astype(HIGH), give_to, -1)
    top = near_total[:half] + above_b.astype(HIGH) + below_a.astype(HIGH)
    bottom = near_total[half:] + below_b.astype(HIGH) + above_a.astype(HIGH)
    total = jnp.concatenate([top, bottom], axis=0).astype(LOW)
    total = jnp.dot(order, total, preferred_element_type=HIGH)
    return sum_along_z(total).astype(LOW)


def solution(mesh):
    torus = Mesh(
        mesh.devices.reshape(mesh.shape["groups"], 4, 16, 2), ("groups", "ep_0", "ep_1", "ep_2")
    )
    placed = (
        P(GROUPS_EP, None),
        P(GROUPS_EP, None),
        P(GROUPS_EP, None),
        P(None, EP),
        P(None, EP),
        P(EP, None),
    )
    return jax.shard_map(layer, mesh=torus, in_specs=placed, out_specs=P(GROUPS_EP, None), check_vma=False)
```
